8 devices in a mesh: replica: 4 (over z, y, x), data: 2 (over core).
Axes of the slice: x: 2, y: 2, z: 1, core: 2. Of those that a mesh axis runs over, the one named last changes fastest.
Arguments:
- w_one: bfloat16 [3, 1920, 7680], replicated
- w_two: bfloat16 [3, 7680, 1920], replicated
- x_in: bfloat16 [24, 2, 64, 1920], P(('replica', 'data'))
- dy_in: bfloat16 [24, 2, 64, 1920], P(('replica', 'data'))
Outputs:
- output 1: bfloat16 [3, 1920, 7680], replicated
- output 2: bfloat16 [3, 7680, 1920], replicated
- output 3: bfloat16 [24, 2, 64, 1920], P(('replica', 'data'))
All inputs are finite; a program needn't handle non-finite values.
Results may differ from the reference program's by a relative error of at most 0.0193242.
Values are sent between devices in bfloat16 or wider.
A program may use at most 1.5 GiB of HBM per device.

```python
import jax
import jax.numpy as jnp
from jax import lax

N_REPLICA = 4
N_DATA = 2
D_MODEL = 1920
D_FF = 7680
LAYERS = 3
MICROBATCHES = 3
MB_SEQS = 2
SEQ_LEN = 64


def setup_inputs(seed: int = 0) -> dict:
    base_key = jax.random.key(seed)
    k_x, k_dy, k_one, k_two = jax.random.split(base_key, 4)
    row_count = N_REPLICA * N_DATA * MICROBATCHES
    shape_x = (row_count, MB_SEQS, SEQ_LEN, D_MODEL)
    x_in = jax.random.normal(k_x, shape_x, jnp.float32).astype(jnp.bfloat16)
    dy_in = jax.random.normal(k_dy, shape_x, jnp.float32).astype(jnp.bfloat16)
    w_one = (jax.random.normal(k_one, (LAYERS, D_MODEL, D_FF), jnp.float32) * D_MODEL ** -0.5).astype(jnp.bfloat16)
    w_two = (jax.random.normal(k_two, (LAYERS, D_FF, D_MODEL), jnp.float32) * D_FF ** -0.5).astype(jnp.bfloat16)
    return {"w_one": w_one, "w_two": w_two, "x_in": x_in, "dy_in": dy_in}


def gelu_tanh(value):
    return jax.nn.gelu(value, approximate=True)


def block_forward(hidden, weights):
    w_up, w_down = weights
    pre_act = jnp.dot(hidden, w_up, preferred_element_type=jnp.float32).astype(jnp.bfloat16)
    gelu_out = gelu_tanh(pre_act.astype(jnp.float32)).astype(jnp.bfloat16)
    new_hidden = (hidden.astype(jnp.float32) + jnp.dot(gelu_out, w_down, preferred_element_type=jnp.float32)).astype(jnp.bfloat16)
    return new_hidden, (hidden, pre_act, gelu_out)


def block_backward(upstream, block_data):
    w_up, w_down, hidden, pre_act, gelu_out = block_data
    grad_b = upstream.astype(jnp.bfloat16)
    d_two = jnp.dot(gelu_out.T, grad_b, preferred_element_type=jnp.float32)
    d_act = jnp.dot(grad_b, w_down.T, preferred_element_type=jnp.float32)
    d_pre = jax.vjp(gelu_tanh, pre_act.astype(jnp.float32))[1](d_act)[0].astype(jnp.bfloat16)
    d_one = jnp.dot(hidden.T, d_pre, preferred_element_type=jnp.float32)
    new_upstream = upstream + jnp.dot(d_pre, w_up.T, preferred_element_type=jnp.float32)
    return new_upstream, (d_one, d_two)


def micro_grads(w_one, w_two, x_mb, dy_mb):
    tokens = x_mb.reshape(-1, D_MODEL)
    _, saved_acts = lax.scan(block_forward, tokens, (w_one, w_two))
    upstream = dy_mb.reshape(-1, D_MODEL).astype(jnp.float32)
    grad_in, (d_one, d_two) = lax.scan(block_backward, upstream, (w_one, w_two) + saved_acts, reverse=True)
    return d_one, d_two, grad_in.astype(jnp.bfloat16).reshape(x_mb.shape)


def reference(w_one, w_two, x_in, dy_in):
    def micro_body(acc_pair, mb_pair):
        acc_one, acc_two = acc_pair
        d_one, d_two, dx_mb = micro_grads(w_one, w_two, mb_pair[0], mb_pair[1])
        return (acc_one + d_one, acc_two + d_two), dx_mb
    start_acc = (jnp.zeros(w_one.shape, jnp.float32), jnp.zeros(w_two.shape, jnp.float32))
    (acc_one, acc_two), dx_out = lax.scan(micro_body, start_acc, (x_in, dy_in))
    return acc_one.astype(jnp.bfloat16), acc_two.astype(jnp.bfloat16), dx_out
```

```python
import jax
import jax.numpy as jnp
from jax import lax
from jax.sharding import PartitionSpec as P


SWAP = ((0, 1), (1, 0))


def gelu_tanh(value):
    return jax.nn.gelu(value, approximate=True)


def swap_cores(value):
    return lax.ppermute(value, "data", SWAP)


def solution(mesh):
    batch_spec = P(("replica", "data"))

    def per_device(w_one, w_two, x_loc, dy_loc):
        layers, model, hidden = w_one.shape
        per = hidden // model // 2
        core = lax.axis_index("data")
        tokens = x_loc.reshape(-1, model)

        def cut(wide, who, axis=1):
            return lax.dynamic_slice_in_dim(wide, who * per * model, per * model, axis)

        def cut_top(w, who, axis):
            start, size = [top, 0, 0], [1, *w.shape[1:]]
            start[axis], size[axis] = who * per * model, per * model
            return lax.dynamic_slice(w, start, size)[0]

        def up(h, w):
            u = jnp.dot(h, w, preferred_element_type=jnp.float32).astype(jnp.bfloat16)
            return u, gelu_tanh(u.astype(jnp.float32)).astype(jnp.bfloat16)

        def grad_one(h, du):
            return jnp.einsum("tm,tf->mf", h, du, preferred_element_type=jnp.float32)

        def grad_two(a, gb):
            return jnp.einsum("tf,tm->fm", a, gb, preferred_element_type=jnp.float32)

        def grad_pre(gb, w, u):
            d_act = jnp.einsum("tm,fm->tf", gb, w, preferred_element_type=jnp.float32)
            return jax.vjp(gelu_tanh, u.astype(jnp.float32))[1](d_act)[0].astype(jnp.bfloat16)

        def grad_in(du, w):
            return jnp.einsum("tf,mf->tm", du, w, preferred_element_type=jnp.float32)

        def part(wide, b):
            return lax.slice_in_dim(wide, b * model, (b + 1) * model, axis=1)

        def own_blocks(dot, away, here):
            got = [swap_cores(dot(part(away, b)).astype(jnp.bfloat16)) for b in range(per)]
            return [(dot(part(here, b)) + got[b].astype(jnp.float32)).astype(jnp.bfloat16) for b in range(per)]

        top = layers - 1
        saved = []
        h = tokens
        for layer in range(top):
            u, a = up(h, w_one[layer])
            saved.append((h, u, a))
            h = (h.astype(jnp.float32) + jnp.dot(a, w_two[layer], preferred_element_type=jnp.float32)).astype(jnp.bfloat16)

        own = {}
        g = dy_loc.reshape(-1, model).astype(jnp.float32)
        gb = g.astype(jnp.bfloat16)
        who = (1 - core, core)
        u_a = [up(h, cut_top(w_one, w, 2)) for w in who]
        got = swap_cores(grad_two(u_a[0][1], gb).astype(jnp.bfloat16))
        send_a = (grad_two(u_a[1][1], gb) + got.astype(jnp.float32)).astype(jnp.bfloat16)
        gb, send_a = lax.optimization_barrier((gb, send_a))
        du = [grad_pre(gb, cut_top(w_two, w, 1), u) for w, (u, _) in zip(who, u_a)]
        own["one", top] = own_blocks(lambda v: grad_one(h, v), *du)
        for w, d in zip(who, du):
            g = g + grad_in(d, cut_top(w_one, w, 2))

        for layer in reversed(range(top)):
            h, u, a = saved[layer]
            gb = g.astype(jnp.bfloat16)
            own["two", layer] = own_blocks(lambda v: grad_two(v, gb), *(cut(a, w) for w in who))
            du = grad_pre(gb, w_two[layer], u)
            own["one", layer] = own_blocks(lambda v: grad_one(h, v), *(cut(du, w) for w in who))
            if layer > 0:
                g = g + grad_in(du, w_one[layer])
        g = g + grad_in(du, w_one[0])
        dx = g.astype(jnp.bfloat16).reshape(x_loc.shape)

        order = [("two", top)]
        for layer in reversed(range(layers)):
            order += [("one", layer)]
        order += [("two", layer) for layer in reversed(range(top))]
        names = [(k, b) for k in order for b in range(per)]
        blocks = [own[k][b] for k, b in names[per:]]
        stages = (names[:per], names[per:-1], names[-1:])
        red_a = lax.psum(send_a, "replica")
        send_b, red_a = lax.optimization_barrier((jnp.concatenate(blocks[:-1], 0), red_a))
        red_b = lax.psum(send_b, "replica")

        outs = {"one": jnp.full(w_one.shape, red_a[0, 0]), "two": jnp.full(w_two.shape, red_a[0, 0])}

        def place(red, stage):
            got = swap_cores(red)
            for src, w in ((red, core), (got, 1 - core)):
                for i, ((kind, layer), b) in enumerate(stage):
                    piece = src[i * model:(i + 1) * model][None]
                    at = (w * per + b) * model
                    start = (layer, 0, at) if kind == "one" else (layer, at, 0)
                    outs[kind] = lax.dynamic_update_slice(outs[kind], piece, start)

        place(red_a, stages[0])
        last, red_b, outs["one"], outs["two"], dx = lax.optimization_barrier((blocks[-1], red_b, outs["one"], outs["two"], dx))
        red_c = lax.psum(last, "replica")
        place(red_b, stages[1])
        red_c, outs["one"], outs["two"] = lax.optimization_barrier((red_c, outs["one"], outs["two"]))
        place(red_c, stages[2])
        return outs["one"], outs["two"], dx

    return jax.shard_map(per_device, mesh=mesh, in_specs=(P(), P(), batch_spec, batch_spec), out_specs=(P(), P(), batch_spec), check_vma=False)
```

```python
import jax
import jax.numpy as jnp
from jax import lax
from jax.sharding import PartitionSpec as P


BOTH = ("replica", "data")


def hop(axes):
    return [(2 * r + c, 2 * (r ^ (1 << axes[c])) + c) for r in range(4) for c in range(2)]


FIRST, SECOND = hop((0, 1)), hop((1, 0))


def gelu_tanh(value):
    return jax.nn.gelu(value, approximate=True)


def add_up(*terms):
    return sum(t.astype(jnp.float32) for t in terms).astype(jnp.bfloat16)


def solution(mesh):
    batch_spec = P(("replica", "data"))

    def per_device(w_one, w_two, x_loc, dy_loc):
        layers, model, hidden = w_one.shape
        size = hidden // 4
        rows = model // 2
        top = layers - 1
        chip, core = lax.axis_index("replica"), lax.axis_index("data")
        pos_x, pos_y = chip % 2, chip // 2
        f = jnp.where(core == 0, pos_x, pos_y)
        s = jnp.where(core == 0, pos_y, pos_x)
        away_send, away_keep = (1 - core) * 2 + 1 - s, (1 - core) * 2 + s
        own_send, own_keep = core * 2 + 1 - f, core * 2 + f

        def swap(value):
            return lax.ppermute(value, "data", [(0, 1), (1, 0)])

        def first(value):
            return lax.ppermute(value, BOTH, FIRST)

        def second(value):
            return lax.ppermute(value, BOTH, SECOND)

        def grad_one(h, du):
            return jnp.einsum("tm,tf->mf", h, du, preferred_element_type=jnp.float32)

        def grad_two(a, gb):
            return jnp.einsum("tf,tm->fm", a, gb, preferred_element_type=jnp.float32)

        def grad_pre(gb, w, u):
            d_act = jnp.einsum("tm,fm->tf", gb, w, preferred_element_type=jnp.float32)
            return jax.vjp(gelu_tanh, u.astype(jnp.float32))[1](d_act)[0].astype(jnp.bfloat16)

        def grad_in(du, w):
            return jnp.einsum("tf,mf->tm", du, w, preferred_element_type=jnp.float32)

        def up(h, w):
            u = jnp.dot(h, w, preferred_element_type=jnp.float32).astype(jnp.bfloat16)
            return u, gelu_tanh(u.astype(jnp.float32)).astype(jnp.bfloat16)

        def cut_top(w, block, axis):
            start, shape = [top, 0, 0], [1, *w.shape[1:]]
            start[axis], shape[axis] = block * size, size
            return lax.dynamic_slice(w, start, shape)[0]

        def cut(wide):
            return lambda block: lax.dynamic_slice_in_dim(wide, block * size, size, 1)

        def chip_sum(dot, away, own):
            return add_up(dot(own), swap(dot(away).astype(jnp.bfloat16)))

        def half(value, which):
            return lax.dynamic_slice_in_dim(value, which * rows, rows, 0)

        def for_second(got_first, keep):
            return add_up(half(keep, 1 - s), half(got_first, 1 - s))

        def summed(got_first, keep, got_second):
            return add_up(half(keep, s), half(got_first, s), got_second)

        saved = []
        h = x_loc.reshape(-1, model)
        for layer in range(top):
            u, a = up(h, w_one[layer])
            saved.append((h, u, a))
            h = (h.astype(jnp.float32) + jnp.dot(a, w_two[layer], preferred_element_type=jnp.float32)).astype(jnp.bfloat16)

        g = dy_loc.reshape(-1, model).astype(jnp.float32)
        gb = g.astype(jnp.bfloat16)
        where = {"away_send": away_send, "own_send": own_send, "away_keep": away_keep, "own_keep": own_keep}

        def top_two(kind, h, gb):
            pairs = [up(h, cut_top(w_one, where[side + kind], 2)) for side in ("away_", "own_")]
            got = swap(grad_two(pairs[0][1], gb).astype(jnp.bfloat16))
            return [u for u, _ in pairs], add_up(grad_two(pairs[1][1], gb), got)

        def top_one(kind, h, gb, u):
            du = [grad_pre(gb, cut_top(w_two, where[side + kind], 1), v) for side, v in zip(("away_", "own_"), u)]
            got = swap(grad_one(h, du[0]).astype(jnp.bfloat16))
            return du, add_up(grad_one(h, du[1]), got)

        gate = lax.optimization_barrier
        u_send, two_send = top_two("send", h, gb)
        two_got = first(two_send)
        gb_one, two_send = gate((gb, two_send))
        du_send, one_send = top_one("send", h, gb_one, u_send)
        one_got = first(one_send)
        h_keep, gb_keep, one_send = gate((h, gb_one, one_send))
        u_keep, two_keep = top_two("keep", h_keep, gb_keep)
        du_keep, one_keep = top_one("keep", h_keep, gb_keep, u_keep)
        two_on = for_second(two_got, two_keep)
        two_got_second = second(two_on)
        du_send, du_keep, two_on, one_keep = gate((du_send, du_keep, two_on, one_keep))
        for kind, du in (("send", du_send), ("keep", du_keep)):
            for side, d in zip(("away_", "own_"), du):
                g = g + grad_in(d, cut_top(w_one, where[side + kind], 2))
        h, u, a = saved[1]
        gb = g.astype(jnp.bfloat16)
        part = cut(a)
        mid_send = chip_sum(lambda v: grad_two(v, gb), part(away_send), part(own_send))
        one_on = for_second(one_got, one_keep)
        mid_got = first(mid_send)
        one_got_second = second(one_on)
        gb_pre, mid_send, one_on = gate((gb, mid_send, one_on))
        du = grad_pre(gb_pre, w_two[1], u)
        two_sum = summed(two_got, two_keep, two_got_second)
        two_pieces = [(two_sum, f, s), (second(two_sum), f, 1 - s), (first(two_sum), 1 - f, s)]
        du, two_sum = gate((du, two_sum))
        part_one = cut(du)
        low_send = chip_sum(lambda v: grad_one(h, v), part_one(away_send), part_one(own_send))
        mid_keep = chip_sum(lambda v: grad_two(v, gb), part(away_keep), part(own_keep))
        low_keep = chip_sum(lambda v: grad_one(h, v), part_one(away_keep), part_one(own_keep))
        low_got = first(low_send)
        du, low_send, mid_keep, low_keep = gate((du, low_send, mid_keep, low_keep))
        g = g + grad_in(du, w_one[1])
        h, u, a = saved[0]
        gb = g.astype(jnp.bfloat16)
        du = grad_pre(gb, w_two[0], u)
        last = []
        for wide, dot in ((a, lambda v: grad_two(v, gb)), (du, lambda v: grad_one(h, v))):
            part = cut(wide)
            got = first(chip_sum(dot, part(away_send), part(own_send)))
            last.append((got, chip_sum(dot, part(away_keep), part(own_keep))))
        g = g + grad_in(du, w_one[0])
        dx = g.astype(jnp.bfloat16).reshape(x_loc.shape)

        outs = {"one": jnp.full(w_one.shape, two_got[0, 0]), "two": jnp.full(w_two.shape, two_got[0, 0])}
        units = [
            ("two", 2, two_got, two_keep, two_got_second),
            ("one", 2, one_got, one_keep, one_got_second),
            ("two", 1, mid_got, mid_keep, None),
            ("one", 1, low_got, low_keep, None),
            ("two", 0, *last[0], None),
            ("one", 0, *last[1], None),
        ]
        for kind, layer, got_first, keep, got_second in units:
            if got_second is None:
                got_second = second(for_second(got_first, keep))
            if (kind, layer) == ("two", 2):
                pieces = two_pieces
            else:
                done = summed(got_first, keep, got_second)
                pieces = [(done, f, s), (second(done), f, 1 - s), (first(done), 1 - f, s)]
            pieces = pieces + [(first(pieces[1][0]), 1 - f, 1 - s)]

            def put(value, block, row):
                at = (layer, row * rows, block * size) if kind == "one" else (layer, block * size + row * rows, 0)
                outs[kind] = lax.dynamic_update_slice(outs[kind], value[None], at)

            for value, block, row in pieces:
                put(value, core * 2 + block, row)
            for (value, _, _), (block, row) in zip(pieces, ((s, f), (s, 1 - f), (1 - s, f), (1 - s, 1 - f))):
                put(swap(value), (1 - core) * 2 + block, row)
        return outs["one"], outs["two"], dx

    return jax.shard_map(per_device, mesh=mesh, in_specs=(P(), P(), batch_spec, batch_spec), out_specs=(P(), P(), batch_spec), check_vma=False)
```
